32 devices in a mesh: dp: 4 (over y, core), expert: 4 (over z), tensor: 2 (over x).
Axes of the slice: x: 2, y: 2, z: 4, core: 2. Of those that a mesh axis runs over, the one named last changes fastest.
Arguments:
- router_input: bfloat16 [1024, 2048], P(('dp', 'expert'), 'tensor'), may hold values from -6 to 6
- router_weight: bfloat16 [2048, 8], replicated, may hold values from -0.125 to 0.125
- expert_ids: int32 [1024, 2], P(('dp', 'expert', 'tensor')), may hold values from 0 to 7, all different within a row; in each aligned block of 32 rows (0 to 31, 32 to 63, ...) at most 9 rows name the same one
- down_weight: bfloat16 [61440, 2048], P(('expert', 'tensor')), may hold values from -0.0625 to 0.0625
- hidden: bfloat16 [4, 72, 61440], P('dp', None, ('expert', 'tensor')), may hold values from -6 to 6
- grad_output: bfloat16 [1024, 2048], P(('dp', 'expert', 'tensor')), may hold values from -4 to 4
Outputs:
- weight_grad: bfloat16 [61440, 2048], P(('expert', 'tensor', 'dp'))
- hidden_grad: bfloat16 [4, 72, 61440], P('dp', None, ('expert', 'tensor'))
- router_grad: float32 [2048, 8], replicated
- input_grad: bfloat16 [1024, 2048], P(('dp', 'expert', 'tensor'))
The draws below stay inside these ranges and needn't reach their ends.
Inputs may be any that keep to these rules, and one draw needn't show every extreme that they name: `expert_ids`: each row names 2 different experts. Within the 32 rows of one device no expert is named more than 9 times, and some device's rows name some expert exactly 9 times.
All inputs are finite; a program needn't handle non-finite values.
Results may differ from the reference program's by a relative error of at most 0.018.
Values may be sent and summed in bfloat16 or wider, within the bound.
A program may use at most 192 MiB of HBM per device.

```python
import math
import jax
import jax.numpy as jnp
import numpy as np
from jax import lax

D = 2048
FF = 7680
EXPERTS = 8
TOPK = 2
TOK_DEV = 32
CAP = 9
SOURCES = 8
TOKENS = 1024
N_DP = 4


def shard_levels(key, shape, split, smallest, largest):
    level, own = 1.0, jax.random.fold_in(key, 6)
    for axis_at, blocks in split:
        draws = jnp.exp(jax.random.uniform(jax.random.fold_in(own, axis_at), (blocks,), jnp.float32, smallest / len(split), largest / len(split)))
        level = level * jnp.repeat(draws, shape[axis_at] // blocks).reshape([-1 if axis == axis_at else 1 for axis in range(len(shape))])
    return level


def deal_out(key, own, number, rows, amount, top, most, slope):
    order = jax.random.permutation(key, amount)
    crowded, common = shares(amount, rows * top, most, slope, True), shares(amount, rows * top, most, slope, False)
    places = jnp.arange(amount)

    def named(tallies, offset_by):
        used = int((tallies > 0).sum())
        fixed = max(1, used // 4)
        shifted = fixed + (places - fixed + offset_by * (used - fixed)) % max(1, amount - fixed)
        return jnp.zeros((amount,), jnp.int32).at[order[jnp.where(places < fixed, places, shifted)]].set(jnp.asarray(tallies, jnp.int32))

    tallies = jnp.where(number % 4 == 0, named(crowded, number // 4), named(common, number - number // 4 - 1))
    mixed = jax.random.permutation(jax.random.fold_in(own, 3), amount)
    donor, receiver = mixed[0:amount // 2 * 2:2], mixed[1:amount // 2 * 2:2]
    slack = jnp.minimum(tallies[donor] - 1, most - tallies[receiver]) // 2
    slack = jnp.where((donor == order[0]) | (receiver == order[0]) | (tallies[receiver] == 0), 0, jnp.maximum(slack, 0))
    shifted = jax.random.randint(jax.random.fold_in(own, 4), (amount // 2,), 0, 1 << 20) % (slack + 1)
    tallies = tallies.at[donor].add(-shifted).at[receiver].add(shifted)
    items = jnp.searchsorted(jnp.cumsum(tallies), jnp.arange(rows * top), side="right").astype(jnp.int32)
    listing = items.reshape(top, rows).T
    listing = listing[jax.random.permutation(jax.random.fold_in(own, 1), rows)]
    offset_by = jax.random.randint(jax.random.fold_in(own, 2), (rows, 1), 0, top)
    return jnp.take_along_axis(listing, (jnp.arange(top)[None, :] + offset_by) % top, axis=1)


def shares(count, total, bound, slope, full):
    weights = [(1 << 20) // math.isqrt(grade ** slope) + 1 for grade in range(1, count + 1)]
    largest = bound if full else min(bound, max(-(-total // count), total * weights[0] // sum(weights)))
    least = 1 if total - largest >= count - 1 else 0
    given, spare = [largest] + [least] * (count - 1), total - largest - least * (count - 1)
    while spare > 0:
        movable = [i for i in range(1, count) if given[i] < largest] or [i for i in range(1, count) if given[i] < bound]
        mass, left = sum([weights[i] for i in movable]), spare
        for i in movable:
            extra = min(bound - given[i], max(1, left * weights[i] // mass), spare)
            given[i] = given[i] + extra
            spare = spare - extra
    return np.array(given)


def centred(stream_key, dims, spread, bound, cuts=(), kind=jnp.bfloat16):
    drawn = jax.random.normal(stream_key, dims, jnp.float32) * spread
    if len(cuts) > 0:
        drawn = shard_levels(stream_key, dims, cuts, -0.22, 0.18) * drawn
    return jnp.clip(drawn, min=-bound, max=bound).astype(kind)


def setup_inputs(seed: int = 0) -> dict:
    splits = jax.random.split(jax.random.key(seed), 7)
    router_input = centred(splits[0], (TOKENS, D), 1.0, 6.0, ((0, 16), (1, 2)))
    router_weight = centred(splits[1], (D, EXPERTS), D ** -0.5, 0.125)
    expert_ids_keys = jax.random.split(jax.random.fold_in(splits[2], 1), TOKENS // TOK_DEV)
    expert_ids_turns = jax.random.permutation(jax.random.fold_in(splits[2], 3), TOKENS // TOK_DEV)
    expert_ids = jax.vmap(lambda own, number: deal_out(jax.random.fold_in(splits[2], 2), own, number, TOK_DEV, EXPERTS, TOPK, CAP, 2))(expert_ids_keys, expert_ids_turns).reshape((TOKENS, TOPK))
    down_weight = centred(splits[3], (EXPERTS * FF, D), FF ** -0.5, 0.0625, ((0, 8),))
    hidden = centred(splits[4], (N_DP, SOURCES * CAP, EXPERTS * FF), 1.0, 6.0, ((0, 4), (2, 8)))
    grad_output = centred(splits[5], (TOKENS, D), 0.25, 4.0, ((0, 32),))
    return dict(router_input=router_input, router_weight=router_weight, expert_ids=expert_ids, down_weight=down_weight, hidden=hidden, grad_output=grad_output)


def reference(router_input, router_weight, expert_ids, down_weight, hidden, grad_output):
    logits = jnp.dot(router_input, router_weight, preferred_element_type=jnp.float32)
    labels = jnp.arange(EXPERTS, dtype=jnp.int32)
    onehot_int = (expert_ids[:, :, None] == labels).astype(jnp.int32)
    onehot = onehot_int.astype(jnp.float32)
    picked = jnp.sum(onehot * logits[:, None, :], axis=2)
    first_gate = jax.nn.sigmoid(picked[:, 0] - picked[:, 1])
    second_gate = jax.nn.sigmoid(picked[:, 1] - picked[:, 0])
    gate_values = jnp.stack([first_gate, second_gate], axis=1)
    gate_low = gate_values.astype(jnp.bfloat16)
    blocks = TOKENS // TOK_DEV
    flat_hits = onehot_int.reshape(blocks, TOK_DEV * TOPK, EXPERTS)
    before = jnp.cumsum(flat_hits, axis=1) - flat_hits
    slot_pos = jnp.sum(before * flat_hits, axis=2).reshape(blocks, TOK_DEV, TOPK)
    slot_ids = jnp.arange(CAP, dtype=jnp.int32)
    dispatch_table = onehot.reshape(blocks, TOK_DEV, TOPK, EXPERTS, 1) * (slot_pos[:, :, :, None, None] == slot_ids).astype(jnp.float32)
    table_groups = dispatch_table.reshape(N_DP, SOURCES, TOK_DEV, TOPK, EXPERTS, CAP)
    grad_groups = grad_output.reshape(N_DP, SOURCES, TOK_DEV, D)
    gate_groups = gate_low.reshape(N_DP, SOURCES, TOK_DEV, TOPK)
    expert_weights = down_weight.reshape(EXPERTS, FF, D)

    def one_expert(pieces):
        expert_grad, expert_gate, expert_hidden, expert_weight = pieces
        expert_image = jnp.dot(expert_grad, expert_weight.T, preferred_element_type=jnp.float32)
        hidden_part = (expert_gate[:, None] * expert_image).astype(jnp.bfloat16)
        gate_part = jnp.sum(expert_hidden.astype(jnp.float32) * expert_image, axis=1)
        gated = (expert_gate[:, None] * expert_grad.astype(jnp.float32)).astype(jnp.bfloat16)
        weight_term = jnp.dot(expert_hidden.T, gated, preferred_element_type=jnp.float32).astype(jnp.bfloat16)
        return hidden_part, gate_part, weight_term

    def one_group(running_total, pieces):
        table_i, grad_i, gate_i, hidden_i = pieces
        slot_table = jnp.sum(table_i, axis=2)
        packed_grad = jnp.einsum("srec,srd->escd", slot_table, grad_i.astype(jnp.float32))
        packed_grad = packed_grad.astype(jnp.bfloat16).reshape(EXPERTS, SOURCES * CAP, D)
        packed_gate = jnp.einsum("srkec,srk->esc", table_i, gate_i.astype(jnp.float32)).reshape(EXPERTS, SOURCES * CAP)
        hidden_split = hidden_i.reshape(SOURCES * CAP, EXPERTS, FF).transpose(1, 0, 2)
        hidden_part, gate_part, weight_term = lax.map(one_expert, (packed_grad, packed_gate, hidden_split, expert_weights))
        running_total = running_total + weight_term.reshape(EXPERTS * FF, D).astype(jnp.float32)
        token_grad = jnp.einsum("srkec,esc->srk", table_i, gate_part.reshape(EXPERTS, SOURCES, CAP))
        hidden_rows = hidden_part.transpose(1, 0, 2).reshape(SOURCES * CAP, EXPERTS * FF)
        return running_total, (hidden_rows, token_grad)

    zero_total = jnp.zeros((EXPERTS * FF, D), jnp.float32)
    running_total, outputs = lax.scan(one_group, zero_total, (table_groups, grad_groups, gate_groups, hidden))
    hidden_grad, token_grad = outputs
    weight_grad = running_total.astype(jnp.bfloat16)
    gate_grad = token_grad.reshape(TOKENS, TOPK)
    mixed_term = jnp.sum(gate_values * gate_grad, axis=1, keepdims=True)
    logit_part = gate_values * (gate_grad - mixed_term)
    logit_grad = jnp.sum(onehot * logit_part[:, :, None], axis=1)
    input_grad = jnp.dot(logit_grad, router_weight.astype(jnp.float32).T, precision=lax.Precision.HIGHEST).astype(jnp.bfloat16)
    router_grad = jnp.dot(router_input.astype(jnp.float32).T, logit_grad, precision=lax.Precision.HIGHEST)
    return weight_grad, hidden_grad, router_grad, input_grad
```

```python
import jax
import jax.numpy as jnp
from jax import lax
from jax.sharding import PartitionSpec as P


def per_device(router_input, router_weight, expert_ids, down_weight, hidden, grad_output):
    token_rows = grad_output.shape[0]
    model_width = grad_output.shape[1]
    expert_count = router_weight.shape[1]
    choose_count = expert_ids.shape[1]
    expert_ranks = lax.axis_size("expert")
    tensor_ranks = lax.axis_size("tensor")
    sources = expert_ranks * tensor_ranks
    spread = sources // expert_count
    capacity = hidden.shape[1] // sources
    full_input = lax.all_to_all(router_input, "tensor", split_axis=0, concat_axis=1, tiled=True)
    logits = jnp.dot(full_input, router_weight, preferred_element_type=jnp.float32)
    labels = jnp.arange(expert_count, dtype=jnp.int32)
    onehot_int = (expert_ids[:, :, None] == labels).astype(jnp.int32)
    onehot = onehot_int.astype(jnp.float32)
    picked = jnp.sum(onehot * logits[:, None, :], axis=2)
    first_gate = jax.nn.sigmoid(picked[:, 0] - picked[:, 1])
    second_gate = jax.nn.sigmoid(picked[:, 1] - picked[:, 0])
    gate_values = jnp.stack([first_gate, second_gate], axis=1)
    gate_low = gate_values.astype(jnp.bfloat16)
    flat_hits = onehot_int.reshape(token_rows * choose_count, expert_count)
    before = jnp.cumsum(flat_hits, axis=0) - flat_hits
    slot_pos = jnp.sum(before * flat_hits, axis=1).reshape(token_rows, choose_count)
    slot_ids = jnp.arange(capacity, dtype=jnp.int32)
    dispatch_table = onehot[:, :, :, None] * (slot_pos[:, :, None, None] == slot_ids).astype(
        jnp.float32
    )
    slot_table = jnp.sum(dispatch_table, axis=1).astype(jnp.bfloat16)
    packed_grad = jnp.einsum(
        "rec,rd->ecd", slot_table, grad_output, preferred_element_type=jnp.float32
    ).astype(jnp.bfloat16)
    packed_gate = jnp.einsum("rkec,rk->ec", dispatch_table, gate_low.astype(jnp.float32)).astype(
        jnp.bfloat16
    )
    send_grad = jnp.repeat(packed_grad, spread, axis=0)
    send_gate = jnp.repeat(packed_gate, spread, axis=0)
    recv_grad, recv_gate = (
        lax.all_to_all(send_grad, ("expert", "tensor"), split_axis=0, concat_axis=0, tiled=True),
        lax.all_to_all(send_gate, ("expert", "tensor"), split_axis=0, concat_axis=0, tiled=True),
    )
    recv_grad = recv_grad.reshape(sources * capacity, model_width)
    recv_gate = recv_gate.reshape(sources * capacity).astype(jnp.float32)
    hidden_rows = hidden[0]
    gated_grad = (recv_gate[:, None] * recv_grad.astype(jnp.float32)).astype(jnp.bfloat16)
    expert_image = lax.dot_general(
        recv_grad, down_weight, (((1,), (1,)), ((), ())), preferred_element_type=jnp.float32
    )
    hidden_part = (recv_gate[:, None] * expert_image).astype(jnp.bfloat16)
    gate_partial = jnp.sum(hidden_rows.astype(jnp.float32) * expert_image, axis=1).reshape(
        sources, capacity
    )
    returned = lax.all_to_all(
        gate_partial, ("expert", "tensor"), split_axis=0, concat_axis=0, tiled=True
    )
    expert_sums = jnp.sum(returned.reshape(expert_count, spread, capacity), axis=1)
    gate_grad = jnp.einsum("rkec,ec->rk", dispatch_table, expert_sums)
    mixed_term = jnp.sum(gate_values * gate_grad, axis=1, keepdims=True)
    logit_part = gate_values * (gate_grad - mixed_term)
    logit_grad = jnp.sum(onehot * logit_part[:, :, None], axis=1)
    input_grad = jnp.dot(
        logit_grad, router_weight.astype(jnp.float32).T, precision=lax.Precision.HIGHEST
    ).astype(jnp.bfloat16)
    router_local = jnp.dot(
        full_input.astype(jnp.float32).T, logit_grad, precision=lax.Precision.HIGHEST
    )
    router_grad = lax.psum(router_local, ("dp", "expert", "tensor"))
    hidden_all = lax.all_to_all(hidden_rows, "dp", split_axis=1, concat_axis=0, tiled=True)
    gated_all = lax.all_gather(gated_grad, "dp", axis=0, tiled=True)
    weight_sum = lax.dot_general(
        hidden_all, gated_all, (((0,), (0,)), ((), ())), preferred_element_type=jnp.float32
    ).astype(jnp.bfloat16)
    return (weight_sum, hidden_part[None], router_grad, input_grad)


def solution(mesh):
    return jax.shard_map(
        per_device,
        mesh=mesh,
        in_specs=(
            P(("dp", "expert"), "tensor"),
            P(),
            P(("dp", "expert", "tensor"), None),
            P(("expert", "tensor"), None),
            P("dp", None, ("expert", "tensor")),
            P(("dp", "expert", "tensor"), None),
        ),
        out_specs=(
            P(("expert", "tensor", "dp"), None),
            P("dp", None, ("expert", "tensor")),
            P(),
            P(("dp", "expert", "tensor"), None),
        ),
        check_vma=False,
    )
```

```python
import functools

import jax
import jax.numpy as jnp
from jax import lax
from jax.experimental import pallas as pl
from jax.experimental.pallas import tpu as pltpu
from jax.sharding import PartitionSpec as P


PAD = 16
LANES = 128
VMEM_LIMIT = 64 * 1000 * 1000
EXACT = lax.Precision.HIGHEST
CONTRACT_LAST = (((1,), (1,)), ((), ()))
CONTRACT_FIRST = (((0,), (0,)), ((), ()))


def iota(shape, axis):
    return lax.broadcasted_iota(jnp.int32, shape, axis)


def exchange_kernel(
    groups, expert_ranks, tensor_ranks, capacity, tile,
    ids_ref, router_weight_ref, grad_ref, router_input_ref, down_ref, hidden_ref,
    hidden_grad_ref, input_grad_ref, router_grad_ref, hidden_all_ref, gated_all_ref,
    weights, hidden_rows, full_input, send_grad, recv_grad, send_gate, recv_gate,
    send_back, recv_back, send_sum, recv_sum, packed, gate_acc,
    weight_sem, hidden_sem, own_sem,
    input_send, input_recv, hidden_send, hidden_recv, grad_send, grad_recv,
    gate_send, gate_recv, gated_send, gated_recv, back_send, back_recv,
    sum_send, sum_recv, whole_send, whole_recv,
):
    f32, bf16 = jnp.float32, jnp.bfloat16
    group = lax.axis_index("dp")
    tensor = lax.axis_index("tensor")
    sources = expert_ranks * tensor_ranks
    source = lax.axis_index("expert") * tensor_ranks + tensor
    devices = groups * sources
    me = group * sources + source
    slots, width = hidden_ref.shape
    part = width // groups
    experts = router_weight_ref.shape[0]
    tokens = grad_ref.shape[0]
    span = router_input_ref.shape[1]
    rows = sources * PAD
    tiles = width // tile

    def place(d, x):
        return {"dp": d, "expert": x // tensor_ranks, "tensor": x % tensor_ranks}

    def remote(src, dst, send, recv, device):
        return pltpu.make_async_remote_copy(
            src_ref=src, dst_ref=dst, send_sem=send, recv_sem=recv,
            device_id=device, device_id_type=pl.DeviceIdType.MESH,
        )

    def weight_copy(i):
        return pltpu.make_async_copy(
            down_ref.at[pl.ds(i * tile, tile)], weights.at[i], weight_sem.at[i]
        )

    barrier = pltpu.get_barrier_semaphore()

    @pl.loop(1, devices)
    def _(k):
        other = (me + k) % devices
        pl.semaphore_signal(
            barrier, inc=1, device_id=place(other // sources, other % sources),
            device_id_type=pl.DeviceIdType.MESH,
        )

    hidden_load = pltpu.make_async_copy(hidden_ref, hidden_rows, hidden_sem)
    hidden_load.start()

    @pl.loop(0, tiles)
    def _(i):
        weight_copy(i).start()

    ids = ids_ref[...]
    labels = iota((tokens, experts), 1)
    first = (ids[:, 0:1] == labels).astype(f32)
    second = (ids[:, 1:2] == labels).astype(f32)
    both = first + second
    earlier = (iota((tokens, tokens), 1) < iota((tokens, tokens), 0)).astype(f32)
    before = jnp.dot(earlier, both, preferred_element_type=f32)
    spread_rows = ((iota((rows, experts), 0) >> 4) == iota((rows, experts), 1)).astype(f32)
    hit = lax.dot_general(spread_rows, both, CONTRACT_LAST, preferred_element_type=f32)
    rank = lax.dot_general(spread_rows, before, CONTRACT_LAST, preferred_element_type=f32)
    slot = (iota((rows, tokens), 0) & (PAD - 1)).astype(f32)
    table = jnp.where((hit > 0.5) & (jnp.abs(rank - slot) < 0.5), 1.0, 0.0).astype(f32)
    send_grad[...] = (
        jnp.dot(table.astype(bf16), grad_ref[...], preferred_element_type=f32)
        .astype(bf16)
        .reshape(send_grad.shape)
    )

    pl.semaphore_wait(barrier, devices - 1)

    input_copies = []
    for k in range(1, tensor_ranks):
        to = (tensor + k) % tensor_ranks
        copy = remote(
            router_input_ref.at[pl.ds(pl.multiple_of(to * tokens, tokens), tokens)],
            full_input.at[tensor], input_send.at[k], input_recv.at[tensor],
            {"tensor": to},
        )
        copy.start()
        input_copies.append(copy)
    own_input = pltpu.make_async_copy(
        router_input_ref.at[pl.ds(pl.multiple_of(tensor * tokens, tokens), tokens)],
        full_input.at[tensor], own_sem.at[0],
    )
    own_input.start()

    grad_copies = []
    for k in range(1, sources):
        to = (source + k) % sources
        copy = remote(
            send_grad.at[to], recv_grad.at[source], grad_send.at[k], grad_recv.at[source],
            place(group, to),
        )
        copy.start()
        grad_copies.append(copy)
    own_grad = pltpu.make_async_copy(send_grad.at[source], recv_grad.at[source], own_sem.at[1])
    own_grad.start()

    hidden_copies = []
    for k in range(1, groups):
        to = (group + k) % groups
        copy = remote(
            hidden_ref.at[:, pl.ds(pl.multiple_of(to * part, LANES), part)],
            hidden_all_ref.at[group], hidden_send.at[k], hidden_recv.at[group],
            {"dp": to},
        )
        copy.start()
        hidden_copies.append(copy)

    own_input.wait()
    for k in range(1, tensor_ranks):
        origin = (tensor + k) % tensor_ranks
        remote(
            router_input_ref.at[pl.ds(0, tokens)], full_input.at[origin], input_send.at[k],
            input_recv.at[origin], {"tensor": origin},
        ).wait_recv()
    logits = jnp.zeros((tokens, experts), f32)
    for h in range(tensor_ranks):
        logits = logits + lax.dot_general(
            full_input[h], router_weight_ref[:, h * span : (h + 1) * span], CONTRACT_LAST,
            preferred_element_type=f32,
        )
    chosen = jnp.sum(first * logits, axis=1, keepdims=True)
    rival = jnp.sum(second * logits, axis=1, keepdims=True)
    first_gate = jax.nn.sigmoid(chosen - rival)
    second_gate = jax.nn.sigmoid(rival - chosen)
    gates = first * first_gate + second * second_gate
    low = gates.astype(bf16).astype(f32)
    gate_rows = lax.dot_general(
        spread_rows, low, CONTRACT_LAST, preferred_element_type=f32
    )
    slot_gate = jnp.sum(table * gate_rows, axis=1, keepdims=True)
    send_gate[...] = jnp.broadcast_to(slot_gate, (rows, LANES)).reshape(send_gate.shape)
    gate_copies = []
    for k in range(1, sources):
        to = (source + k) % sources
        copy = remote(
            send_gate.at[to], recv_gate.at[source], gate_send.at[k], gate_recv.at[source],
            place(group, to),
        )
        copy.start()
        gate_copies.append(copy)
    own_gate = pltpu.make_async_copy(send_gate.at[source], recv_gate.at[source], own_sem.at[2])
    own_gate.start()

    own_grad.wait()
    own_gate.wait()
    for k in range(1, sources):
        origin = (source + k) % sources
        remote(
            send_grad.at[0], recv_grad.at[origin], grad_send.at[k], grad_recv.at[origin],
            place(group, origin),
        ).wait_recv()
        remote(
            send_gate.at[0], recv_gate.at[origin], gate_send.at[k], gate_recv.at[origin],
            place(group, origin),
        ).wait_recv()
    column = iota((slots, rows), 1)
    column_slot = column & (PAD - 1)
    pick = (
        (iota((slots, rows), 0) == capacity * (column >> 4) + column_slot)
        & (column_slot < capacity)
    ).astype(f32)
    pick_low = pick.astype(bf16)
    packed_grad = jnp.dot(
        pick_low, recv_grad[...].reshape(rows, recv_grad.shape[2]), preferred_element_type=f32
    )
    packed[...] = packed_grad.astype(bf16)
    gate_lanes = jnp.dot(
        pick_low, recv_gate[...].reshape(rows, LANES).astype(bf16), preferred_element_type=f32
    )
    gate_column = gate_lanes[:, 0:1]
    gated_all_ref[pl.ds(group, 1)] = (gate_column * packed_grad).astype(bf16)[None]

    core = group % 2
    half = group // 2
    beside = half * 2 + (1 - core)
    across = (1 - half) * 2 + core
    diagonal = (1 - half) * 2 + (1 - core)
    mine = gated_all_ref.at[group]
    to_across = remote(mine, mine, gated_send.at[0], gated_recv.at[group], {"dp": across})
    to_across.start()
    to_beside = remote(mine, mine, gated_send.at[1], gated_recv.at[group], {"dp": beside})
    to_beside.start()

    hidden_load.wait()
    own_hidden = pltpu.make_async_copy(
        hidden_rows.at[:, pl.ds(pl.multiple_of(group * part, LANES), part)],
        hidden_all_ref.at[group], own_sem.at[3],
    )
    own_hidden.start()
    gate_acc[...] = jnp.zeros_like(gate_acc)

    @pl.loop(0, tiles)
    def _(i):
        weight_copy(i).wait()
        at = pl.ds(pl.multiple_of(i * tile, tile), tile)
        image = lax.dot_general(
            packed[...], weights[i], CONTRACT_LAST, preferred_element_type=f32
        )
        hidden_grad_ref[:, at] = (gate_column * image).astype(bf16)
        product = hidden_rows[:, at].astype(f32) * image
        total = product[:, 0:LANES]
        for j in range(1, tile // LANES):
            total = total + product[:, j * LANES : (j + 1) * LANES]
        gate_acc[...] += total

    partial = jnp.broadcast_to(
        jnp.sum(gate_acc[...], axis=1, keepdims=True), (slots, LANES)
    )
    send_back[...] = lax.dot_general(
        pick, partial, CONTRACT_FIRST, precision=EXACT, preferred_element_type=f32
    ).reshape(send_back.shape)
    back_copies = []
    for k in range(1, sources):
        to = (source + k) % sources
        copy = remote(
            send_back.at[to], recv_back.at[source], back_send.at[k], back_recv.at[source],
            place(group, to),
        )
        copy.start()
        back_copies.append(copy)
    own_back = pltpu.make_async_copy(send_back.at[source], recv_back.at[source], own_sem.at[4])
    own_back.start()

    theirs = gated_all_ref.at[across]
    remote(theirs, theirs, gated_send.at[0], gated_recv.at[across], {"dp": across}).wait_recv()
    relay = remote(theirs, theirs, gated_send.at[2], gated_recv.at[across], {"dp": beside})
    relay.start()

    own_back.wait()
    for k in range(1, sources):
        origin = (source + k) % sources
        remote(
            send_back.at[0], recv_back.at[origin], back_send.at[k], back_recv.at[origin],
            place(group, origin),
        ).wait_recv()
    returned = recv_back[...].reshape(rows, LANES)[:, 0:1]
    gate_grad = lax.dot_general(
        table * returned, spread_rows, CONTRACT_FIRST, precision=EXACT, preferred_element_type=f32
    )
    mixed = jnp.sum(gates * gate_grad, axis=1, keepdims=True)
    logit_grad = gates * (gate_grad - mixed)
    chunk = experts // groups
    block = (span * tensor_ranks) // sources
    for h in range(tensor_ranks):
        local = lax.dot_general(
            logit_grad, full_input[h].astype(f32), CONTRACT_FIRST, precision=EXACT,
            preferred_element_type=f32,
        )
        for b in range(span // block):
            x = h * (span // block) + b
            for d in range(groups):
                send_sum[d * sources + x] = local[
                    d * chunk : (d + 1) * chunk, b * block : (b + 1) * block
                ]

    def sum_copy(k, to, slot_at):
        return remote(
            send_sum.at[to], recv_sum.at[slot_at], sum_send.at[k], sum_recv.at[slot_at],
            place(to // sources, to % sources),
        )

    def whole_copy(k, to, slot_at):
        return remote(
            router_grad_ref.at[slot_at], router_grad_ref.at[slot_at], whole_send.at[k],
            whole_recv.at[slot_at], place(to // sources, to % sources),
        )

    @pl.loop(1, devices)
    def _(k):
        sum_copy(k, (me + k) % devices, me).start()

    recv_sum[pl.ds(me, 1)] = send_sum[pl.ds(me, 1)]
    input_grad_ref[...] = jnp.dot(
        logit_grad, router_weight_ref[...].astype(f32), precision=EXACT,
        preferred_element_type=f32,
    ).astype(bf16)

    @pl.loop(1, devices)
    def _(k):
        origin = (me + k) % devices
        sum_copy(k, origin, origin).wait_recv()

    router_grad_ref[pl.ds(me, 1)] = jnp.sum(recv_sum[...], axis=0, keepdims=True)

    @pl.loop(1, devices)
    def _(k):
        whole_copy(k, (me + k) % devices, me).start()

    @pl.loop(1, devices)
    def _(k):
        origin = (me + k) % devices
        whole_copy(k, origin, origin).wait_recv()

    own_hidden.wait()
    for k in range(1, groups):
        origin = (group + k) % groups
        remote(
            hidden_ref.at[:, pl.ds(0, part)], hidden_all_ref.at[origin], hidden_send.at[k],
            hidden_recv.at[origin], {"dp": origin},
        ).wait_recv()
    for origin in (beside, diagonal):
        slab = gated_all_ref.at[origin]
        remote(
            slab, slab, gated_send.at[1], gated_recv.at[origin], {"dp": beside}
        ).wait_recv()
    for copy in input_copies + grad_copies + hidden_copies + gate_copies + back_copies:
        copy.wait_send()
    for copy in (to_across, to_beside, relay):
        copy.wait_send()

    @pl.loop(1, devices)
    def _(k):
        sum_copy(k, (me + k) % devices, me).wait_send()
        whole_copy(k, (me + k) % devices, me).wait_send()


def weight_kernel(hidden_ref, gated_ref, out_ref):
    out_ref[...] = lax.dot_general(
        hidden_ref[...], gated_ref[...], CONTRACT_FIRST, preferred_element_type=jnp.float32
    ).astype(out_ref.dtype)


def by_kernels(router_input, router_weight, expert_ids, down_weight, hidden, grad_output):
    f32, bf16 = jnp.float32, jnp.bfloat16
    tokens, model = grad_output.shape
    experts = router_weight.shape[1]
    groups = lax.axis_size("dp")
    expert_ranks = lax.axis_size("expert")
    tensor_ranks = lax.axis_size("tensor")
    sources = expert_ranks * tensor_ranks
    devices = groups * sources
    slots, width = hidden.shape[1:]
    tile = tile_of(width)
    span = router_input.shape[1]
    part = width // groups
    vmem = pl.BlockSpec(memory_space=pltpu.VMEM)
    hbm = pl.BlockSpec(memory_space=pl.ANY)
    dma = pltpu.SemaphoreType.DMA
    piece = (devices, experts // groups, model // sources)
    hidden_grad, input_grad, router_parts, hidden_all, gated_all = pl.pallas_call(
        functools.partial(
            exchange_kernel, groups, expert_ranks, tensor_ranks, slots // sources, tile
        ),
        out_shape=(
            jax.ShapeDtypeStruct((slots, width), bf16),
            jax.ShapeDtypeStruct((tokens, model), bf16),
            jax.ShapeDtypeStruct(piece, f32),
            jax.ShapeDtypeStruct((groups, slots, part), bf16),
            jax.ShapeDtypeStruct((groups, slots, model), bf16),
        ),
        in_specs=[vmem, vmem, vmem, vmem, hbm, hbm],
        out_specs=(vmem, vmem, vmem, hbm, vmem),
        scratch_shapes=[
            pltpu.VMEM((width // tile, tile, model), bf16),
            pltpu.VMEM((slots, width), bf16),
            pltpu.VMEM((tensor_ranks, tokens, span), bf16),
            pltpu.VMEM((sources, PAD, model), bf16),
            pltpu.VMEM((sources, PAD, model), bf16),
            pltpu.VMEM((sources, PAD, LANES), f32),
            pltpu.VMEM((sources, PAD, LANES), f32),
            pltpu.VMEM((sources, PAD, LANES), f32),
            pltpu.VMEM((sources, PAD, LANES), f32),
            pltpu.VMEM(piece, f32),
            pltpu.VMEM(piece, f32),
            pltpu.VMEM((slots, model), bf16),
            pltpu.VMEM((slots, LANES), f32),
            dma((width // tile,)),
            dma,
            dma((5,)),
            dma((tensor_ranks,)), dma((tensor_ranks,)),
            dma((groups,)), dma((groups,)),
            dma((sources,)), dma((sources,)),
            dma((sources,)), dma((sources,)),
            dma((3,)), dma((groups,)),
            dma((sources,)), dma((sources,)),
            dma((devices,)), dma((devices,)),
            dma((devices,)), dma((devices,)),
        ],
        compiler_params=pltpu.CompilerParams(
            collective_id=0, has_side_effects=True, vmem_limit_bytes=VMEM_LIMIT
        ),
        name="exchange",
    )(expert_ids, router_weight.T, grad_output, router_input, down_weight, hidden[0])
    step = 384 if part % 384 == 0 else LANES
    weight_grad = pl.pallas_call(
        weight_kernel,
        out_shape=jax.ShapeDtypeStruct((part, model), bf16),
        grid=(part // step,),
        in_specs=[
            pl.BlockSpec((groups * slots, step), lambda i: (0, i)),
            pl.BlockSpec((groups * slots, model), lambda i: (0, 0)),
        ],
        out_specs=pl.BlockSpec((step, model), lambda i: (i, 0)),
        name="weight_grad",
    )(hidden_all.reshape(groups * slots, part), gated_all.reshape(groups * slots, model))
    router_grad = (
        router_parts.reshape(groups, sources, experts // groups, model // sources)
        .transpose(1, 3, 0, 2)
        .reshape(model, experts)
    )
    return weight_grad, hidden_grad[None], router_grad, input_grad


def tile_of(width):
    for tile in (512, 384, 256):
        if width % tile == 0:
            return tile
    return LANES


def kernels_fit(router_input, router_weight, expert_ids, down_weight, hidden, grad_output):
    groups = lax.axis_size("dp")
    sources = lax.axis_size("expert") * lax.axis_size("tensor")
    slots, width = hidden.shape[1:]
    tokens, model = grad_output.shape
    experts = router_weight.shape[1]
    return (
        groups == 4
        and sources == experts
        and experts % groups == 0
        and slots % 8 == 0
        and slots // sources <= PAD
        and tokens % 16 == 0
        and width % (groups * LANES) == 0
        and model % (sources * LANES) == 0
        and 2 * (width * model + 4 * slots * width + 8 * slots * model) < 48 * 1000 * 1000
    )


def per_device(*arrays):
    return by_kernels(*arrays) if kernels_fit(*arrays) else by_collectives(*arrays)


def by_collectives(router_input, router_weight, expert_ids, down_weight, hidden, grad_output):
    token_rows = grad_output.shape[0]
    model_width = grad_output.shape[1]
    expert_count = router_weight.shape[1]
    choose_count = expert_ids.shape[1]
    expert_ranks = lax.axis_size("expert")
    tensor_ranks = lax.axis_size("tensor")
    sources = expert_ranks * tensor_ranks
    spread = sources // expert_count
    capacity = hidden.shape[1] // sources
    full_input = lax.all_to_all(router_input, "tensor", split_axis=0, concat_axis=1, tiled=True)
    logits = jnp.dot(full_input, router_weight, preferred_element_type=jnp.float32)
    labels = jnp.arange(expert_count, dtype=jnp.int32)
    onehot_int = (expert_ids[:, :, None] == labels).astype(jnp.int32)
    onehot = onehot_int.astype(jnp.float32)
    picked = jnp.sum(onehot * logits[:, None, :], axis=2)
    first_gate = jax.nn.sigmoid(picked[:, 0] - picked[:, 1])
    second_gate = jax.nn.sigmoid(picked[:, 1] - picked[:, 0])
    gate_values = jnp.stack([first_gate, second_gate], axis=1)
    gate_low = gate_values.astype(jnp.bfloat16)
    flat_hits = onehot_int.reshape(token_rows * choose_count, expert_count)
    before = jnp.cumsum(flat_hits, axis=0) - flat_hits
    slot_pos = jnp.sum(before * flat_hits, axis=1).reshape(token_rows, choose_count)
    slot_ids = jnp.arange(capacity, dtype=jnp.int32)
    dispatch_table = onehot[:, :, :, None] * (slot_pos[:, :, None, None] == slot_ids).astype(
        jnp.float32
    )
    slot_table = jnp.sum(dispatch_table, axis=1).astype(jnp.bfloat16)
    packed_grad = jnp.einsum(
        "rec,rd->ecd", slot_table, grad_output, preferred_element_type=jnp.float32
    ).astype(jnp.bfloat16)
    packed_gate = jnp.einsum("rkec,rk->ec", dispatch_table, gate_low.astype(jnp.float32)).astype(
        jnp.bfloat16
    )
    send_grad = jnp.repeat(packed_grad, spread, axis=0)
    send_gate = jnp.repeat(packed_gate, spread, axis=0)
    recv_grad, recv_gate = (
        lax.all_to_all(send_grad, ("expert", "tensor"), split_axis=0, concat_axis=0, tiled=True),
        lax.all_to_all(send_gate, ("expert", "tensor"), split_axis=0, concat_axis=0, tiled=True),
    )
    recv_grad = recv_grad.reshape(sources * capacity, model_width)
    recv_gate = recv_gate.reshape(sources * capacity).astype(jnp.float32)
    hidden_rows = hidden[0]
    gated_grad = (recv_gate[:, None] * recv_grad.astype(jnp.float32)).astype(jnp.bfloat16)
    expert_image = lax.dot_general(
        recv_grad, down_weight, (((1,), (1,)), ((), ())), preferred_element_type=jnp.float32
    )
    hidden_part = (recv_gate[:, None] * expert_image).astype(jnp.bfloat16)
    gate_partial = jnp.sum(hidden_rows.astype(jnp.float32) * expert_image, axis=1).reshape(
        sources, capacity
    )
    returned = lax.all_to_all(
        gate_partial, ("expert", "tensor"), split_axis=0, concat_axis=0, tiled=True
    )
    expert_sums = jnp.sum(returned.reshape(expert_count, spread, capacity), axis=1)
    gate_grad = jnp.einsum("rkec,ec->rk", dispatch_table, expert_sums)
    mixed_term = jnp.sum(gate_values * gate_grad, axis=1, keepdims=True)
    logit_part = gate_values * (gate_grad - mixed_term)
    logit_grad = jnp.sum(onehot * logit_part[:, :, None], axis=1)
    input_grad = jnp.dot(
        logit_grad, router_weight.astype(jnp.float32).T, precision=lax.Precision.HIGHEST
    ).astype(jnp.bfloat16)
    router_local = jnp.dot(
        full_input.astype(jnp.float32).T, logit_grad, precision=lax.Precision.HIGHEST
    )
    router_grad = lax.psum(router_local, ("dp", "expert", "tensor"))
    hidden_all = lax.all_to_all(hidden_rows, "dp", split_axis=1, concat_axis=0, tiled=True)
    gated_all = lax.all_gather(gated_grad, "dp", axis=0, tiled=True)
    weight_sum = lax.dot_general(
        hidden_all, gated_all, (((0,), (0,)), ((), ())), preferred_element_type=jnp.float32
    ).astype(jnp.bfloat16)
    return (weight_sum, hidden_part[None], router_grad, input_grad)


def solution(mesh):
    return jax.shard_map(
        per_device,
        mesh=mesh,
        in_specs=(
            P(("dp", "expert"), "tensor"),
            P(),
            P(("dp", "expert", "tensor"), None),
            P(("expert", "tensor"), None),
            P("dp", None, ("expert", "tensor")),
            P(("dp", "expert", "tensor"), None),
        ),
        out_specs=(
            P(("expert", "tensor", "dp"), None),
            P("dp", None, ("expert", "tensor")),
            P(),
            P(("dp", "expert", "tensor"), None),
        ),
        check_vma=False,
    )
```

```python
import functools

import jax
import jax.numpy as jnp
from jax import lax
from jax.experimental import pallas as pl
from jax.experimental.pallas import tpu as pltpu
from jax.sharding import PartitionSpec as P


PAD = 16
PIECES = 4
LANES = 128
VMEM_LIMIT = 64 * 1000 * 1000
EXACT = lax.Precision.HIGHEST
CONTRACT_LAST = (((1,), (1,)), ((), ()))
CONTRACT_FIRST = (((0,), (0,)), ((), ()))


def iota(shape, axis):
    return lax.broadcasted_iota(jnp.int32, shape, axis)


def exchange_kernel(
    groups, expert_ranks, tensor_ranks, capacity, tile,
    ids_ref, router_weight_ref, grad_ref, router_input_ref, down_ref, hidden_ref,
    hidden_grad_ref, input_grad_ref, router_grad_ref, hidden_all_ref, gated_out_ref,
    weights, hidden_rows, full_input, send_grad, recv_grad, send_gate, recv_gate,
    send_back, recv_back, send_sum, recv_sum, packed, gate_acc, gated_all_ref, hidden_out, image_acc,
    weight_sem, hidden_sem, own_sem, piece_sem, out_sem, gated_out,
    input_send, input_recv, hidden_send, hidden_recv, grad_send, grad_recv,
    gate_send, gate_recv, gated_send, gated_recv, back_send, back_recv,
    sum_send, sum_recv, whole_send, whole_recv,
):
    f32, bf16 = jnp.float32, jnp.bfloat16
    group = lax.axis_index("dp")
    tensor = lax.axis_index("tensor")
    sources = expert_ranks * tensor_ranks
    source = lax.axis_index("expert") * tensor_ranks + tensor
    devices = groups * sources
    me = group * sources + source
    slots, width = hidden_ref.shape
    part = width // groups
    experts = router_weight_ref.shape[0]
    tokens = grad_ref.shape[0]
    span = router_input_ref.shape[1]
    rows = sources * PAD
    tiles = width // tile

    def place(d, x):
        return {"dp": d, "expert": x // tensor_ranks, "tensor": x % tensor_ranks}

    def remote(src, dst, send, recv, device):
        return pltpu.make_async_remote_copy(
            src_ref=src, dst_ref=dst, send_sem=send, recv_sem=recv,
            device_id=device, device_id_type=pl.DeviceIdType.MESH,
        )

    def weight_copy(i):
        return pltpu.make_async_copy(
            down_ref.at[pl.ds(i * tile, tile)], weights.at[i], weight_sem.at[i]
        )

    barrier = pltpu.get_barrier_semaphore()

    @pl.loop(1, devices)
    def _(k):
        other = (me + k) % devices
        pl.semaphore_signal(
            barrier, inc=1, device_id=place(other // sources, other % sources),
            device_id_type=pl.DeviceIdType.MESH,
        )

    hidden_load = pltpu.make_async_copy(hidden_ref, hidden_rows, hidden_sem)
    hidden_load.start()

    @pl.loop(0, tiles)
    def _(i):
        weight_copy(i).start()

    labels = iota((experts, tokens), 0)
    same = (iota((tokens, tokens), 0) == iota((tokens, tokens), 1)).astype(f32)
    first = lax.dot_general(
        same, (ids_ref[0:1, :] == labels).astype(f32), CONTRACT_LAST, preferred_element_type=f32
    )
    second = lax.dot_general(
        same, (ids_ref[1:2, :] == labels).astype(f32), CONTRACT_LAST, preferred_element_type=f32
    )
    both = first + second
    earlier = (iota((tokens, tokens), 1) < iota((tokens, tokens), 0)).astype(f32)
    before = jnp.dot(earlier, both, preferred_element_type=f32)
    spread_rows = ((iota((rows, experts), 0) >> 4) == iota((rows, experts), 1)).astype(f32)
    hit = lax.dot_general(spread_rows, both, CONTRACT_LAST, preferred_element_type=f32)
    rank = lax.dot_general(spread_rows, before, CONTRACT_LAST, preferred_element_type=f32)
    slot = (iota((rows, tokens), 0) & (PAD - 1)).astype(f32)
    table = jnp.where((hit > 0.5) & (jnp.abs(rank - slot) < 0.5), 1.0, 0.0).astype(f32)
    wide = grad_ref.shape[1] // PIECES
    for p in range(PIECES):
        send_grad[p] = (
            jnp.dot(
                table.astype(bf16), grad_ref[:, p * wide : (p + 1) * wide],
                preferred_element_type=f32,
            )
            .astype(bf16)
            .reshape(send_grad.shape[1:])
        )

    pl.semaphore_wait(barrier, devices - 1)

    grad_copies = []

    def dispatch(p):
        for k in range(1, sources):
            to = (source + k) % sources
            copy = remote(
                send_grad.at[p, to], recv_grad.at[p, source], grad_send.at[p * sources + k],
                grad_recv.at[p * sources + source], place(group, to),
            )
            copy.start()
            grad_copies.append(copy)
        own = pltpu.make_async_copy(
            send_grad.at[p, source], recv_grad.at[p, source], piece_sem.at[p]
        )
        own.start()
        return own

    own_grads = [dispatch(0)]
    input_copies = []
    for k in range(1, tensor_ranks):
        to = (tensor + k) % tensor_ranks
        copy = remote(
            router_input_ref.at[pl.ds(pl.multiple_of(to * tokens, tokens), tokens)],
            full_input.at[tensor], input_send.at[k], input_recv.at[tensor],
            {"tensor": to},
        )
        copy.start()
        input_copies.append(copy)
    own_input = pltpu.make_async_copy(
        router_input_ref.at[pl.ds(pl.multiple_of(tensor * tokens, tokens), tokens)],
        full_input.at[tensor], own_sem.at[0],
    )
    own_input.start()

    for p in range(1, PIECES):
        own_grads.append(dispatch(p))

    hidden_copies = []
    for k in range(1, groups):
        to = (group + k) % groups
        copy = remote(
            hidden_ref.at[:, pl.ds(pl.multiple_of(to * part, LANES), part)],
            hidden_all_ref.at[group], hidden_send.at[k], hidden_recv.at[group],
            {"dp": to},
        )
        copy.start()
        hidden_copies.append(copy)

    column = iota((slots, rows), 1)
    column_slot = column & (PAD - 1)
    pick = (
        (iota((slots, rows), 0) == capacity * (column >> 4) + column_slot)
        & (column_slot < capacity)
    ).astype(f32)
    pick_low = pick.astype(bf16)

    def receive(p):
        own_grads[p].wait()
        for k in range(1, sources):
            origin = (source + k) % sources
            remote(
                send_grad.at[p, 0], recv_grad.at[p, origin], grad_send.at[p * sources + k],
                grad_recv.at[p * sources + origin], place(group, origin),
            ).wait_recv()
        packed[p] = jnp.dot(
            pick_low, recv_grad[p].reshape(rows, wide), preferred_element_type=f32
        ).astype(bf16)

    def image_piece(p, i):
        return lax.dot_general(
            packed[p], weights[i, :, p * wide : (p + 1) * wide], CONTRACT_LAST,
            preferred_element_type=f32,
        )

    receive(0)

    @pl.loop(0, tiles)
    def _(i):
        weight_copy(i).wait()
        image_acc[i] = image_piece(0, i)

    own_input.wait()
    for k in range(1, tensor_ranks):
        origin = (tensor + k) % tensor_ranks
        remote(
            router_input_ref.at[pl.ds(0, tokens)], full_input.at[origin], input_send.at[k],
            input_recv.at[origin], {"tensor": origin},
        ).wait_recv()
    logits = jnp.zeros((tokens, experts), f32)
    for h in range(tensor_ranks):
        logits = logits + lax.dot_general(
            full_input[h], router_weight_ref[:, h * span : (h + 1) * span], CONTRACT_LAST,
            preferred_element_type=f32,
        )
    chosen = jnp.sum(first * logits, axis=1, keepdims=True)
    rival = jnp.sum(second * logits, axis=1, keepdims=True)
    first_gate = jax.nn.sigmoid(chosen - rival)
    second_gate = jax.nn.sigmoid(rival - chosen)
    gates = first * first_gate + second * second_gate
    low = gates.astype(bf16).astype(f32)
    gate_rows = lax.dot_general(
        spread_rows, low, CONTRACT_LAST, preferred_element_type=f32
    )
    slot_gate = jnp.sum(table * gate_rows, axis=1, keepdims=True)
    send_gate[...] = jnp.broadcast_to(slot_gate, (rows, LANES)).reshape(send_gate.shape)
    gate_copies = []
    for k in range(1, sources):
        to = (source + k) % sources
        copy = remote(
            send_gate.at[to], recv_gate.at[source], gate_send.at[k], gate_recv.at[source],
            place(group, to),
        )
        copy.start()
        gate_copies.append(copy)
    own_gate = pltpu.make_async_copy(send_gate.at[source], recv_gate.at[source], own_sem.at[2])
    own_gate.start()

    for p in range(1, PIECES - 1):
        receive(p)

        @pl.loop(0, tiles)
        def _(i):
            image_acc[i] += image_piece(p, i)

    receive(PIECES - 1)
    own_gate.wait()
    for k in range(1, sources):
        origin = (source + k) % sources
        remote(
            send_gate.at[0], recv_gate.at[origin], gate_send.at[k], gate_recv.at[origin],
            place(group, origin),
        ).wait_recv()
    gate_lanes = jnp.dot(
        pick_low, recv_gate[...].reshape(rows, LANES).astype(bf16), preferred_element_type=f32
    )
    gate_column = gate_lanes[:, 0:1]
    for p in range(PIECES):
        gated_all_ref[pl.ds(group, 1), :, p * wide : (p + 1) * wide] = (
            gate_column * packed[p].astype(f32)
        ).astype(bf16)[None]

    core = group % 2
    half = group // 2
    beside = half * 2 + (1 - core)
    across = (1 - half) * 2 + core
    diagonal = (1 - half) * 2 + (1 - core)
    mine = gated_all_ref.at[group]
    to_across = remote(mine, mine, gated_send.at[0], gated_recv.at[group], {"dp": across})
    to_across.start()
    to_beside = remote(mine, mine, gated_send.at[1], gated_recv.at[group], {"dp": beside})
    to_beside.start()

    def gated_copy(d):
        return pltpu.make_async_copy(gated_all_ref.at[d], gated_out_ref.at[d], gated_out.at[d])

    gated_copy(group).start()
    hidden_load.wait()
    own_hidden = pltpu.make_async_copy(
        hidden_rows.at[:, pl.ds(pl.multiple_of(group * part, LANES), part)],
        hidden_all_ref.at[group], own_sem.at[3],
    )
    own_hidden.start()
    gate_acc[...] = jnp.zeros_like(gate_acc)

    @pl.loop(0, tiles)
    def _(i):
        at = pl.ds(pl.multiple_of(i * tile, tile), tile)
        image = image_acc[i] + image_piece(PIECES - 1, i)
        hidden_out[:, at] = (gate_column * image).astype(bf16)
        product = hidden_rows[:, at].astype(f32) * image
        total = product[:, 0:LANES]
        for j in range(1, tile // LANES):
            total = total + product[:, j * LANES : (j + 1) * LANES]
        gate_acc[...] += total

    hidden_store = pltpu.make_async_copy(hidden_out, hidden_grad_ref, out_sem)
    hidden_store.start()
    partial = jnp.broadcast_to(
        jnp.sum(gate_acc[...], axis=1, keepdims=True), (slots, LANES)
    )
    send_back[...] = lax.dot_general(
        pick, partial, CONTRACT_FIRST, precision=EXACT, preferred_element_type=f32
    ).reshape(send_back.shape)
    back_copies = []
    for k in range(1, sources):
        to = (source + k) % sources
        copy = remote(
            send_back.at[to], recv_back.at[source], back_send.at[k], back_recv.at[source],
            place(group, to),
        )
        copy.start()
        back_copies.append(copy)
    own_back = pltpu.make_async_copy(send_back.at[source], recv_back.at[source], own_sem.at[4])
    own_back.start()

    theirs = gated_all_ref.at[across]
    remote(theirs, theirs, gated_send.at[0], gated_recv.at[across], {"dp": across}).wait_recv()
    relay = remote(theirs, theirs, gated_send.at[2], gated_recv.at[across], {"dp": beside})
    relay.start()
    gated_copy(across).start()

    own_back.wait()
    for k in range(1, sources):
        origin = (source + k) % sources
        remote(
            send_back.at[0], recv_back.at[origin], back_send.at[k], back_recv.at[origin],
            place(group, origin),
        ).wait_recv()
    returned = recv_back[...].reshape(rows, LANES)[:, 0:1]
    gate_grad = lax.dot_general(
        table * returned, spread_rows, CONTRACT_FIRST, precision=EXACT, preferred_element_type=f32
    )
    mixed = jnp.sum(gates * gate_grad, axis=1, keepdims=True)
    logit_grad = gates * (gate_grad - mixed)
    chunk = experts // groups
    block = (span * tensor_ranks) // sources
    for h in range(tensor_ranks):
        local = lax.dot_general(
            logit_grad, full_input[h].astype(f32), CONTRACT_FIRST, precision=EXACT,
            preferred_element_type=f32,
        )
        for b in range(span // block):
            x = h * (span // block) + b
            for d in range(groups):
                send_sum[d * sources + x] = local[
                    d * chunk : (d + 1) * chunk, b * block : (b + 1) * block
                ]

    def sum_copy(k, to, slot_at):
        return remote(
            send_sum.at[to], recv_sum.at[slot_at], sum_send.at[k], sum_recv.at[slot_at],
            place(to // sources, to % sources),
        )

    def whole_copy(k, to, slot_at):
        return remote(
            router_grad_ref.at[slot_at], router_grad_ref.at[slot_at], whole_send.at[k],
            whole_recv.at[slot_at], place(to // sources, to % sources),
        )

    @pl.loop(1, devices)
    def _(k):
        sum_copy(k, (me + k) % devices, me).start()

    recv_sum[pl.ds(me, 1)] = send_sum[pl.ds(me, 1)]
    input_grad_ref[...] = jnp.dot(
        logit_grad, router_weight_ref[...].astype(f32), precision=EXACT,
        preferred_element_type=f32,
    ).astype(bf16)

    @pl.loop(1, devices)
    def _(k):
        origin = (me + k) % devices
        sum_copy(k, origin, origin).wait_recv()

    router_grad_ref[pl.ds(me, 1)] = jnp.sum(recv_sum[...], axis=0, keepdims=True)

    @pl.loop(1, devices)
    def _(k):
        whole_copy(k, (me + k) % devices, me).start()

    @pl.loop(1, devices)
    def _(k):
        origin = (me + k) % devices
        whole_copy(k, origin, origin).wait_recv()

    own_hidden.wait()
    for k in range(1, groups):
        origin = (group + k) % groups
        remote(
            hidden_ref.at[:, pl.ds(0, part)], hidden_all_ref.at[origin], hidden_send.at[k],
            hidden_recv.at[origin], {"dp": origin},
        ).wait_recv()
    for origin in (beside, diagonal):
        slab = gated_all_ref.at[origin]
        remote(
            slab, slab, gated_send.at[1], gated_recv.at[origin], {"dp": beside}
        ).wait_recv()
        gated_copy(origin).start()
    for copy in input_copies + grad_copies + hidden_copies + gate_copies + back_copies:
        copy.wait_send()
    for copy in (to_across, to_beside, relay):
        copy.wait_send()
    for d in (group, beside, across, diagonal):
        gated_copy(d).wait()
    hidden_store.wait()

    @pl.loop(1, devices)
    def _(k):
        sum_copy(k, (me + k) % devices, me).wait_send()
        whole_copy(k, (me + k) % devices, me).wait_send()


def weight_kernel(
    sources, hidden_ref, gated_ref, hidden_grad_ref, input_grad_ref, router_ref,
    out_ref, hidden_grad_out, input_grad_out, router_out,
):
    hidden_grad_out[...] = hidden_grad_ref[...]

    @pl.when(pl.program_id(0) == 0)
    def _():
        input_grad_out[...] = input_grad_ref[...]
        pieces, chunk, block = router_ref.shape
        for piece in range(pieces):
            d, x = piece // sources, piece % sources
            router_out[d * chunk : (d + 1) * chunk, x * block : (x + 1) * block] = router_ref[
                piece
            ]

    out_ref[...] = lax.dot_general(
        hidden_ref[...], gated_ref[...], CONTRACT_FIRST, preferred_element_type=jnp.float32
    ).astype(out_ref.dtype)


def by_kernels(router_input, router_weight, expert_ids, down_weight, hidden, grad_output):
    f32, bf16 = jnp.float32, jnp.bfloat16
    tokens, model = grad_output.shape
    experts = router_weight.shape[1]
    groups = lax.axis_size("dp")
    expert_ranks = lax.axis_size("expert")
    tensor_ranks = lax.axis_size("tensor")
    sources = expert_ranks * tensor_ranks
    devices = groups * sources
    slots, width = hidden.shape[1:]
    tile = tile_of(width)
    span = router_input.shape[1]
    part = width // groups
    vmem = pl.BlockSpec(memory_space=pltpu.VMEM)
    hbm = pl.BlockSpec(memory_space=pl.ANY)
    dma = pltpu.SemaphoreType.DMA
    piece = (devices, experts // groups, model // sources)
    hidden_grad, input_grad, router_parts, hidden_all, gated_all = pl.pallas_call(
        functools.partial(
            exchange_kernel, groups, expert_ranks, tensor_ranks, slots // sources, tile
        ),
        out_shape=(
            jax.ShapeDtypeStruct((slots, width), bf16),
            jax.ShapeDtypeStruct((tokens, model), bf16),
            jax.ShapeDtypeStruct(piece, f32),
            jax.ShapeDtypeStruct((groups, slots, part), bf16),
            jax.ShapeDtypeStruct((groups, slots, model), bf16),
        ),
        in_specs=[vmem, vmem, vmem, vmem, hbm, hbm],
        out_specs=(hbm, vmem, vmem, hbm, hbm),
        scratch_shapes=[
            pltpu.VMEM((width // tile, tile, model), bf16),
            pltpu.VMEM((slots, width), bf16),
            pltpu.VMEM((tensor_ranks, tokens, span), bf16),
            pltpu.VMEM((PIECES, sources, PAD, model // PIECES), bf16),
            pltpu.VMEM((PIECES, sources, PAD, model // PIECES), bf16),
            pltpu.VMEM((sources, PAD, LANES), f32),
            pltpu.VMEM((sources, PAD, LANES), f32),
            pltpu.VMEM((sources, PAD, LANES), f32),
            pltpu.VMEM((sources, PAD, LANES), f32),
            pltpu.VMEM(piece, f32),
            pltpu.VMEM(piece, f32),
            pltpu.VMEM((PIECES, slots, model // PIECES), bf16),
            pltpu.VMEM((slots, LANES), f32),
            pltpu.VMEM((groups, slots, model), bf16),
            pltpu.VMEM((slots, width), bf16),
            pltpu.VMEM((width // tile, slots, tile), f32),
            dma((width // tile,)),
            dma,
            dma((5,)),
            dma((PIECES,)),
            dma,
            dma((groups,)),
            dma((tensor_ranks,)), dma((tensor_ranks,)),
            dma((groups,)), dma((groups,)),
            dma((PIECES * sources,)), dma((PIECES * sources,)),
            dma((sources,)), dma((sources,)),
            dma((3,)), dma((groups,)),
            dma((sources,)), dma((sources,)),
            dma((devices,)), dma((devices,)),
            dma((devices,)), dma((devices,)),
        ],
        compiler_params=pltpu.CompilerParams(
            collective_id=0, has_side_effects=True, vmem_limit_bytes=VMEM_LIMIT
        ),
        name="exchange",
    )(expert_ids.T, router_weight.T, grad_output, router_input, down_weight, hidden[0])
    step = 384 if part % 384 == 0 else LANES
    steps = part // step
    slab = width // steps
    weight_grad, hidden_grad, input_grad, router_grad = pl.pallas_call(
        functools.partial(weight_kernel, sources),
        out_shape=(
            jax.ShapeDtypeStruct((part, model), bf16),
            jax.ShapeDtypeStruct((slots, width), bf16),
            jax.ShapeDtypeStruct((tokens, model), bf16),
            jax.ShapeDtypeStruct((experts, model), f32),
        ),
        grid=(steps,),
        in_specs=[
            pl.BlockSpec((groups * slots, step), lambda i: (0, i)),
            pl.BlockSpec((groups * slots, model), lambda i: (0, 0)),
            pl.BlockSpec((slots, slab), lambda i: (0, i)),
            pl.BlockSpec((tokens, model), lambda i: (0, 0)),
            pl.BlockSpec(piece, lambda i: (0, 0, 0)),
        ],
        out_specs=(
            pl.BlockSpec((step, model), lambda i: (i, 0)),
            pl.BlockSpec((slots, slab), lambda i: (0, i)),
            pl.BlockSpec((tokens, model), lambda i: (0, 0)),
            pl.BlockSpec((experts, model), lambda i: (0, 0)),
        ),
        name="weight_grad",
    )(
        hidden_all.reshape(groups * slots, part),
        gated_all.reshape(groups * slots, model),
        hidden_grad, input_grad, router_parts,
    )
    return weight_grad, hidden_grad[None], router_grad.T, input_grad


def tile_of(width):
    for tile in (512, 384, 256):
        if width % tile == 0:
            return tile
    return LANES


def kernels_fit(router_input, router_weight, expert_ids, down_weight, hidden, grad_output):
    groups = lax.axis_size("dp")
    sources = lax.axis_size("expert") * lax.axis_size("tensor")
    slots, width = hidden.shape[1:]
    tokens, model = grad_output.shape
    experts = router_weight.shape[1]
    return (
        groups == 4
        and sources == experts
        and experts % groups == 0
        and slots % 8 == 0
        and slots // sources <= PAD
        and tokens % 16 == 0
        and width % (groups * LANES) == 0
        and model % (sources * LANES) == 0
        and model % (PIECES * LANES) == 0
        and 2 * (width * model + 4 * slots * width + 8 * slots * model) < 48 * 1000 * 1000
    )


def per_device(*arrays):
    return by_kernels(*arrays) if kernels_fit(*arrays) else by_collectives(*arrays)


def by_collectives(router_input, router_weight, expert_ids, down_weight, hidden, grad_output):
    token_rows = grad_output.shape[0]
    model_width = grad_output.shape[1]
    expert_count = router_weight.shape[1]
    choose_count = expert_ids.shape[1]
    expert_ranks = lax.axis_size("expert")
    tensor_ranks = lax.axis_size("tensor")
    sources = expert_ranks * tensor_ranks
    spread = sources // expert_count
    capacity = hidden.shape[1] // sources
    full_input = lax.all_to_all(router_input, "tensor", split_axis=0, concat_axis=1, tiled=True)
    logits = jnp.dot(full_input, router_weight, preferred_element_type=jnp.float32)
    labels = jnp.arange(expert_count, dtype=jnp.int32)
    onehot_int = (expert_ids[:, :, None] == labels).astype(jnp.int32)
    onehot = onehot_int.astype(jnp.float32)
    picked = jnp.sum(onehot * logits[:, None, :], axis=2)
    first_gate = jax.nn.sigmoid(picked[:, 0] - picked[:, 1])
    second_gate = jax.nn.sigmoid(picked[:, 1] - picked[:, 0])
    gate_values = jnp.stack([first_gate, second_gate], axis=1)
    gate_low = gate_values.astype(jnp.bfloat16)
    flat_hits = onehot_int.reshape(token_rows * choose_count, expert_count)
    before = jnp.cumsum(flat_hits, axis=0) - flat_hits
    slot_pos = jnp.sum(before * flat_hits, axis=1).reshape(token_rows, choose_count)
    slot_ids = jnp.arange(capacity, dtype=jnp.int32)
    dispatch_table = onehot[:, :, :, None] * (slot_pos[:, :, None, None] == slot_ids).astype(
        jnp.float32
    )
    slot_table = jnp.sum(dispatch_table, axis=1).astype(jnp.bfloat16)
    packed_grad = jnp.einsum(
        "rec,rd->ecd", slot_table, grad_output, preferred_element_type=jnp.float32
    ).astype(jnp.bfloat16)
    packed_gate = jnp.einsum("rkec,rk->ec", dispatch_table, gate_low.astype(jnp.float32)).astype(
        jnp.bfloat16
    )
    send_grad = jnp.repeat(packed_grad, spread, axis=0)
    send_gate = jnp.repeat(packed_gate, spread, axis=0)
    recv_grad, recv_gate = (
        lax.all_to_all(send_grad, ("expert", "tensor"), split_axis=0, concat_axis=0, tiled=True),
        lax.all_to_all(send_gate, ("expert", "tensor"), split_axis=0, concat_axis=0, tiled=True),
    )
    recv_grad = recv_grad.reshape(sources * capacity, model_width)
    recv_gate = recv_gate.reshape(sources * capacity).astype(jnp.float32)
    hidden_rows = hidden[0]
    gated_grad = (recv_gate[:, None] * recv_grad.astype(jnp.float32)).astype(jnp.bfloat16)
    expert_image = lax.dot_general(
        recv_grad, down_weight, (((1,), (1,)), ((), ())), preferred_element_type=jnp.float32
    )
    hidden_part = (recv_gate[:, None] * expert_image).astype(jnp.bfloat16)
    gate_partial = jnp.sum(hidden_rows.astype(jnp.float32) * expert_image, axis=1).reshape(
        sources, capacity
    )
    returned = lax.all_to_all(
        gate_partial, ("expert", "tensor"), split_axis=0, concat_axis=0, tiled=True
    )
    expert_sums = jnp.sum(returned.reshape(expert_count, spread, capacity), axis=1)
    gate_grad = jnp.einsum("rkec,ec->rk", dispatch_table, expert_sums)
    mixed_term = jnp.sum(gate_values * gate_grad, axis=1, keepdims=True)
    logit_part = gate_values * (gate_grad - mixed_term)
    logit_grad = jnp.sum(onehot * logit_part[:, :, None], axis=1)
    input_grad = jnp.dot(
        logit_grad, router_weight.astype(jnp.float32).T, precision=lax.Precision.HIGHEST
    ).astype(jnp.bfloat16)
    router_local = jnp.dot(
        full_input.astype(jnp.float32).T, logit_grad, precision=lax.Precision.HIGHEST
    )
    router_grad = lax.psum(router_local, ("dp", "expert", "tensor"))
    hidden_all = lax.all_to_all(hidden_rows, "dp", split_axis=1, concat_axis=0, tiled=True)
    gated_all = lax.all_gather(gated_grad, "dp", axis=0, tiled=True)
    weight_sum = lax.dot_general(
        hidden_all, gated_all, (((0,), (0,)), ((), ())), preferred_element_type=jnp.float32
    ).astype(jnp.bfloat16)
    return (weight_sum, hidden_part[None], router_grad, input_grad)


def solution(mesh):
    return jax.shard_map(
        per_device,
        mesh=mesh,
        in_specs=(
            P(("dp", "expert"), "tensor"),
            P(),
            P(("dp", "expert", "tensor"), None),
            P(("expert", "tensor"), None),
            P("dp", None, ("expert", "tensor")),
            P(("dp", "expert", "tensor"), None),
        ),
        out_specs=(
            P(("expert", "tensor", "dp"), None),
            P("dp", None, ("expert", "tensor")),
            P(),
            P(("dp", "expert", "tensor"), None),
        ),
        check_vma=False,
    )
```
